256 devices in a mesh: gx: 4 (over z_hi, core), gy: 16 (over z_lo, y), gz: 4 (over x).
Axes of the slice: x: 4, y: 4, z: 8 (z_hi: 2, z_lo: 4; z = z_hi * 4 + z_lo), core: 2. Of those that a mesh axis runs over, the one named last changes fastest.
Arguments:
- random_vectors: float32 [64, 128, 128, 128], P('gx', 'gy', 'gz'), may hold values from -6 to 6
- potential: float32 [64, 128, 128], P('gx', 'gy', 'gz'), may hold values from -2.5 to 2.5
Outputs:
- moments: float32 [9, 128], replicated
- chebyshev_vector: float32 [64, 128, 128, 128], P('gx', 'gy', 'gz')
The draws below stay inside these ranges and needn't reach their ends.
All inputs are finite; a program needn't handle non-finite values.
Results may differ from the reference program's by a relative error of at most 0.0001.
Values sent between devices are 32-bit elements; how exact they have to be, the bound alone decides.
A program may use at most 64 MiB of HBM per device.

```python
import math
import jax
import jax.numpy as jnp
from jax import lax

R = 128
ITERS = 4
NX = 64
NY = 128
NZ = 128


def level_of(key, extent, pieces, low, largest):
    factor_of, own = 1.0, jax.random.fold_in(key, 6)
    for dim, parts in pieces:
        heights = jnp.exp(jax.random.uniform(jax.random.fold_in(own, dim), (parts,), jnp.float32, low / len(pieces), largest / len(pieces)))
        factor_of = factor_of * jnp.repeat(heights, extent[dim] // parts).reshape([-1 if axis == dim else 1 for axis in range(len(extent))])
    return factor_of


def bell_draw(own_key, extent, deviation, bound, split=(), held_as=jnp.bfloat16):
    values = deviation * jax.random.normal(own_key, extent, jnp.float32)
    if split:
        values = values * level_of(own_key, extent, split, -0.22, 0.18)
    return jnp.clip(values, -bound, bound).astype(held_as)


def setup_inputs(seed: int = 0) -> dict:
    splits = jax.random.split(jax.random.key(seed), 3)
    random_vectors = bell_draw(splits[0], (NX, NY, NZ, R), 1.0, 6.0, ((0, 4), (1, 16), (2, 4)), jnp.float32)
    potential = jnp.clip(jax.random.uniform(splits[1], (NX, NY, NZ), jnp.float32, -2.5, 2.5) * level_of(splits[1], (NX, NY, NZ), ((0, 4), (1, 16), (2, 4)), -0.4, 0.0), -2.5, 2.5)
    return dict(random_vectors=random_vectors, potential=potential)


def apply_hamiltonian(field, potential):
    beside = jnp.roll(field, 1, 0) + jnp.roll(field, -1, 0)
    beside = beside + jnp.roll(field, 1, 1) + jnp.roll(field, -1, 1)
    beside = beside + jnp.roll(field, 1, 2) + jnp.roll(field, -1, 2)
    return (potential[..., None] * field - beside) / 9.0


def reference(random_vectors, potential):
    width = math.gcd(R, 16)
    groups = R // width

    def one_block(start):
        previous = start
        current = apply_hamiltonian(start, potential)
        sums = [jnp.sum(start * start, axis=(0, 1, 2)), jnp.sum(start * current, axis=(0, 1, 2))]
        keep = current
        for index in range(1, 2 * ITERS):
            following = 2.0 * apply_hamiltonian(current, potential) - previous
            sums.append(jnp.sum(start * following, axis=(0, 1, 2)))
            previous, current = current, following
            if index + 1 == ITERS:
                keep = following
        return jnp.stack(sums), keep

    blocks = jnp.moveaxis(random_vectors.reshape(NX, NY, NZ, groups, width), 3, 0)
    sums, keeps = lax.map(one_block, blocks)
    moments = jnp.moveaxis(sums, 0, 1).reshape(2 * ITERS + 1, R) / (NX * NY * NZ)
    chebyshev_vector = jnp.moveaxis(keeps, 0, 3).reshape(NX, NY, NZ, R)
    return moments, chebyshev_vector
```

```python
import jax
import jax.numpy as jnp
from jax import lax
from jax.experimental import pallas as pl
from jax.experimental.pallas import tpu as pltpu
from jax.sharding import PartitionSpec as P

LX, LY, LZ, R = 16, 8, 32, 128
PX, PY, PZ = LX + 2, LY + 2, 40
ITERS = 4
SITES = 64 * 128 * 128
MESH = pl.DeviceIdType.MESH
XLO, XHI, YLO, YHI, ZLO, ZHI = range(6)


def kernel(v_ref, pot_ref, mom_ref, out_ref, t0, t1, t2, t3, t4, w, zsend, zrecv,
           part, bufa, bufb, load_sem, store_sem, send_sem, recv_sem, asend, arecv, bsend, brecv):
    gx, gy, gz = lax.axis_index("gx"), lax.axis_index("gy"), lax.axis_index("gz")
    t = [t0, t1, t2, t3, t4]
    flat = [r.reshape(PX * PY * PZ, R) for r in t[:4]] + [t4]

    def dev(dx, dy, dz):
        return (lax.rem(gx + dx + 4, 4), lax.rem(gy + dy + 16, 16), lax.rem(gz + dz + 4, 4))

    def inside(ref, x0, x1):
        return ref.at[pl.ds(x0 + 1, x1 - x0), pl.ds(1, LY), pl.ds(0, LZ), :]

    load = pltpu.make_async_copy(v_ref, inside(t0, 0, LX), load_sem)
    load.start()

    row_y = lax.rem(gy, 4)
    row_z = gy // 4
    mine_a = row_y * 4 + gz
    mine_b = row_z * 4 + gx
    peers_a = [(gx, row_z * 4 + lax.rem(row_y + i // 4, 4), lax.rem(gz + i % 4, 4)) for i in range(1, 16)]
    peers_b = [(lax.rem(gx + i % 4, 4), lax.rem(row_z + i // 4, 4) * 4 + row_y, gz) for i in range(1, 16)]
    near = [dev(-1, 0, 0), dev(1, 0, 0), dev(0, -1, 0), dev(0, 1, 0), dev(0, 0, -1), dev(0, 0, 1)]
    barrier = pltpu.get_barrier_semaphore()
    for peer in near + peers_a + peers_b:
        pl.semaphore_signal(barrier, inc=1, device_id=peer, device_id_type=MESH)

    pot_t = jnp.transpose(pot_ref[...].reshape(LX * LY, LZ)) * (2.0 / 9.0)
    for k in range(LX * LY):
        w[k * LZ:(k + 1) * LZ, :] = jnp.broadcast_to(pot_t[:, k:k + 1], (LZ, R))

    pl.semaphore_wait(barrier, 36)
    load.wait()

    def remote(src, dst, n, way, peer):
        return pltpu.make_async_remote_copy(
            src_ref=src, dst_ref=dst, send_sem=send_sem.at[n, way], recv_sem=recv_sem.at[n, way],
            device_id=peer, device_id_type=MESH)

    def xcopies(n):
        r = t[n]
        return [
            remote(r.at[LX, pl.ds(1, LY), pl.ds(0, LZ), :], r.at[0, pl.ds(1, LY), pl.ds(0, LZ), :], n, XLO, near[1]),
            remote(r.at[1, pl.ds(1, LY), pl.ds(0, LZ), :], r.at[LX + 1, pl.ds(1, LY), pl.ds(0, LZ), :], n, XHI, near[0]),
        ]

    def ycopies(n):
        r = t[n]
        return [
            remote(r.at[pl.ds(1, LX), LY, pl.ds(0, LZ), :], r.at[pl.ds(1, LX), 0, pl.ds(0, LZ), :], n, YLO, near[3]),
            remote(r.at[pl.ds(1, LX), 1, pl.ds(0, LZ), :], r.at[pl.ds(1, LX), LY + 1, pl.ds(0, LZ), :], n, YHI, near[2]),
        ]

    def zcopies(n):
        return [
            remote(zsend.at[n, 0], zrecv.at[n, 0], n, ZLO, near[5]),
            remote(zsend.at[n, 1], zrecv.at[n, 1], n, ZHI, near[4]),
        ]

    def zpack(n):
        f = flat[n]
        for x in range(LX):
            base = ((x + 1) * PY + 1) * PZ
            zsend[n, 0, x] = f[pl.ds(base + LZ - 1, LY, stride=PZ), :]
            zsend[n, 1, x] = f[pl.ds(base, LY, stride=PZ), :]

    def zunpack(n):
        f = flat[n]
        for x in range(LX):
            base = ((x + 1) * PY + 1) * PZ
            f[pl.ds(base - 1, LY, stride=PZ), :] = zrecv[n, 0, x]
            f[pl.ds(base + LZ, LY, stride=PZ), :] = zrecv[n, 1, x]

    def columns(n, x, ys, sums):
        cur, nxt = flat[n], flat[n + 1]
        for y in ys:
            base = pl.multiple_of(((x + 1) * PY + y + 1) * PZ, 8)
            wb = pl.multiple_of((x * LY + y) * LZ, 8)
            c = cur[pl.ds(base, LZ), :]
            beside = cur[pl.ds(base - PY * PZ, LZ), :] + cur[pl.ds(base + PY * PZ, LZ), :]
            beside = beside + (cur[pl.ds(base - PZ, LZ), :] + cur[pl.ds(base + PZ, LZ), :])
            beside = beside + (cur[pl.ds(base - 1, LZ), :] + cur[pl.ds(base + 1, LZ), :])
            new = w[pl.ds(wb, LZ), :] * c - (2.0 / 9.0) * beside
            if n == 0:
                new = 0.5 * new
                sums = (sums[0], sums[1], sums[2] + c * c)
            else:
                new = new - flat[n - 1][pl.ds(base, LZ), :]
            nxt[pl.ds(wb if n == ITERS - 1 else base, LZ), :] = new
            sums = (sums[0] + new * c, sums[1] + new * new, sums[2])
        return sums

    copies = []
    for c in xcopies(0) + ycopies(0):
        c.start()
        copies.append(c)
    zpack(0)
    for c in zcopies(0):
        c.start()
        copies.append(c)

    rows = [None] * 9
    for n in range(ITERS):
        for c in zcopies(n) + ycopies(n) + xcopies(n):
            c.wait_recv()
        zunpack(n)
        zero = jnp.zeros((LZ, R), jnp.float32)
        sums = (zero, zero, zero)
        for x in (0, LX - 1):
            sums = columns(n, x, range(LY), sums)
        if n < ITERS - 1:
            for c in xcopies(n + 1):
                c.start()
                copies.append(c)
        sums = lax.fori_loop(1, LX - 1, lambda x, s: columns(n, x, (0, LY - 1), s), sums)
        if n < ITERS - 1:
            for c in ycopies(n + 1):
                c.start()
                copies.append(c)
        sums = lax.fori_loop(1, LX - 1, lambda x, s: columns(n, x, range(1, LY - 1), s), sums)
        if n < ITERS - 1:
            zpack(n + 1)
            for c in zcopies(n + 1):
                c.start()
                copies.append(c)
        if n == 0:
            rows[0] = jnp.sum(sums[2], axis=0, keepdims=True)
        rows[2 * n + 1] = jnp.sum(sums[0], axis=0, keepdims=True)
        rows[2 * n + 2] = jnp.sum(sums[1], axis=0, keepdims=True)

    store = pltpu.make_async_copy(t4.reshape(LX, LY, LZ, R), out_ref, store_sem)
    store.start()

    def gather(peers, buf, mine, ssem, rsem, size):
        outs = []
        for i, peer in enumerate(peers):
            c = pltpu.make_async_remote_copy(
                src_ref=part, dst_ref=buf.at[mine], send_sem=ssem.at[i], recv_sem=rsem.at[mine],
                device_id=peer, device_id_type=MESH)
            c.start()
            outs.append(c)
        return outs

    def arrive(peers_index, buf, mine, rsem, ssem):
        for i in range(1, 16):
            slot = peers_index(i)
            pltpu.make_async_remote_copy(
                src_ref=part, dst_ref=buf.at[slot], send_sem=ssem.at[0], recv_sem=rsem.at[slot],
                device_id=(gx, gy, gz), device_id_type=MESH).wait_recv()

    part[...] = jnp.concatenate(rows + [jnp.zeros((7, R), jnp.float32)], axis=0)
    bufa[mine_a] = part[...]
    outs = gather(peers_a, bufa, mine_a, asend, arecv, 16)
    arrive(lambda i: lax.rem(row_y + i // 4, 4) * 4 + lax.rem(gz + i % 4, 4), bufa, mine_a, arecv, asend)
    for c in outs:
        c.wait_send()
    total = bufa[0]
    for i in range(1, 16):
        total = total + bufa[i]
    part[...] = total
    bufb[mine_b] = total
    outs = gather(peers_b, bufb, mine_b, bsend, brecv, 16)
    arrive(lambda i: lax.rem(row_z + i // 4, 4) * 4 + lax.rem(gx + i % 4, 4), bufb, mine_b, brecv, bsend)
    for c in outs:
        c.wait_send()
    total = bufb[0]
    for i in range(1, 16):
        total = total + bufb[i]
    order = lax.broadcasted_iota(jnp.int32, (16, R), 0)
    base = jnp.where(order % 2 == 0, total[0:1, :], total[1:2, :])
    full = jnp.where(order < 2, total, 2.0 * total - base) * (1.0 / SITES)
    mom_ref[...] = full[:9, :]
    for c in copies:
        c.wait_send()
    store.wait()


def shards(random_vectors, potential):
    padded = pltpu.VMEM((PX, PY, PZ, R), jnp.float32)
    dma = pltpu.SemaphoreType.DMA
    return pl.pallas_call(
        kernel,
        out_shape=(jax.ShapeDtypeStruct((9, R), jnp.float32),
                   jax.ShapeDtypeStruct((LX, LY, LZ, R), jnp.float32)),
        in_specs=[pl.BlockSpec(memory_space=pl.ANY), pl.BlockSpec(memory_space=pltpu.VMEM)],
        out_specs=(pl.BlockSpec(memory_space=pltpu.VMEM), pl.BlockSpec(memory_space=pl.ANY)),
        scratch_shapes=[padded] * 4 + [
            pltpu.VMEM((LX * LY * LZ, R), jnp.float32),
            pltpu.VMEM((LX * LY * LZ, R), jnp.float32),
            pltpu.VMEM((ITERS, 2, LX, LY, R), jnp.float32),
            pltpu.VMEM((ITERS, 2, LX, LY, R), jnp.float32),
            pltpu.VMEM((16, R), jnp.float32),
            pltpu.VMEM((16, 16, R), jnp.float32),
            pltpu.VMEM((16, 16, R), jnp.float32),
            dma, dma, dma((ITERS, 6)), dma((ITERS, 6)),
            dma((16,)), dma((16,)), dma((16,)), dma((16,)),
        ],
        compiler_params=pltpu.CompilerParams(
            collective_id=0, has_side_effects=True, vmem_limit_bytes=48 * 1024 * 1024),
    )(random_vectors, potential)


def solution(mesh):
    placed = (P("gx", "gy", "gz", None), P("gx", "gy", "gz"))
    return jax.shard_map(
        shards, mesh=mesh, in_specs=placed, out_specs=(P(), P("gx", "gy", "gz", None)), check_vma=False)
```

```python
import jax
import jax.numpy as jnp
from jax import lax
from jax.experimental import pallas as pl
from jax.experimental.pallas import tpu as pltpu
from jax.sharding import PartitionSpec as P

LX, LY, LZ, R = 16, 8, 32, 128
PX, PY, PZ = LX + 2, LY + 2, 40
HALF = LX // 2
ITERS = 4
SITES = 64 * 128 * 128
MESH = pl.DeviceIdType.MESH
FARA, FARB, NEAR, YLO, YHI, ZLO, ZHI, WAYS = 0, 1, 2, 3, 5, 7, 9, 11


def kernel(v_ref, pot_ref, mom_ref, out_ref, t0, t1, t2, t3, w, pot, zsend, zrecv, relay,
           part, bufa, bufb, load_sem, pot_sem, send_sem, recv_sem, relay_send, relay_recv,
           asend, arecv, bsend, brecv):
    gx, gy, gz = lax.axis_index("gx"), lax.axis_index("gy"), lax.axis_index("gz")
    t = [t0, t1, t2, t3]
    flat = [r.reshape(PX * PY * PZ, R) for r in t] + [out_ref.reshape(LX * LY * LZ, R)]
    par = lax.rem(gx, 2)
    row_y = lax.rem(gy, 4)
    row_z = gy // 4
    far_plane, near_plane = 1 + par * (LX - 1), LX - par * (LX - 1)
    far_halo, near_halo = par * (LX + 1), (1 - par) * (LX + 1)
    x_half = [(1 - par) * HALF, par * HALF]

    def plane(k):
        return k * par + (LX - 1 - k) * (1 - par)

    load = pltpu.make_async_copy(v_ref, t0.at[pl.ds(1, LX), pl.ds(1, LY), pl.ds(0, LZ), :], load_sem)
    load.start()
    load_pot = pltpu.make_async_copy(pot_ref, pot, pot_sem)
    load_pot.start()

    mine_a = row_y * 4 + gz
    mine_b = row_z * 4 + gx
    peers_a = [(gx, row_z * 4 + lax.rem(row_y + i // 4, 4), lax.rem(gz + i % 4, 4)) for i in range(1, 16)]
    peers_b = [(lax.rem(gx + i % 4, 4), lax.rem(row_z + i // 4, 4) * 4 + row_y, gz) for i in range(1, 16)]
    far = (lax.rem(gx + 2 * par + 3, 4), gy, gz)
    near = (gx + 1 - 2 * par, gy, gz)
    ydn, yup = (gx, lax.rem(gy + 15, 16), gz), (gx, lax.rem(gy + 1, 16), gz)
    zdn, zup = (gx, gy, lax.rem(gz + 3, 4)), (gx, gy, lax.rem(gz + 1, 4))
    barrier = pltpu.get_barrier_semaphore()
    side = 1 - 2 * lax.rem(row_y, 2)
    edge = (row_y == 0) | (row_y == 3)
    beside = (gx, gy + side, gz)
    diag = (far[0], gy + side, gz)
    greeted = [far, near, ydn, yup, zdn, zup, diag] + peers_a + peers_b
    for peer in greeted:
        pl.semaphore_signal(barrier, inc=1, device_id=peer, device_id_type=MESH)

    load_pot.wait()
    pot_t = jnp.transpose(pot[...].reshape(LX * LY, LZ)) * (2.0 / 9.0)
    for k in range(LX * LY):
        w[k * LZ:(k + 1) * LZ, :] = jnp.broadcast_to(pot_t[:, k:k + 1], (LZ, R))

    load.wait()
    pl.semaphore_wait(barrier, len(greeted))

    def remote(src, dst, n, way, peer):
        return pltpu.make_async_remote_copy(
            src_ref=src, dst_ref=dst, send_sem=send_sem.at[n, way], recv_sem=recv_sem.at[n, way],
            device_id=peer, device_id_type=MESH)

    def far_copy(n, j):
        ys, zs = pl.ds(1 + j * LY // 2, LY // 2), pl.ds(0, LZ)
        return remote(t[n].at[far_plane, ys, zs, :], t[n].at[(1 - par) * (LX + 1), ys, zs, :], n, FARA + j, far)

    def hop_copy(n):
        return pltpu.make_async_remote_copy(
            src_ref=t[n].at[far_plane, pl.ds(1 + n % 2 * LY // 2, LY // 2), pl.ds(0, LZ), :], dst_ref=relay.at[n],
            send_sem=send_sem.at[n, FARA + n % 2], recv_sem=relay_recv.at[n],
            device_id=beside, device_id_type=MESH)

    def pass_copy(n):
        return pltpu.make_async_remote_copy(
            src_ref=relay.at[n],
            dst_ref=t[n].at[(1 - par) * (LX + 1), pl.ds(1 + n % 2 * LY // 2, LY // 2), pl.ds(0, LZ), :],
            send_sem=relay_send.at[n], recv_sem=recv_sem.at[n, FARA + n % 2],
            device_id=diag, device_id_type=MESH)

    def send_far(n, j):
        if j != n % 2:
            send([far_copy(n, j)])
        else:
            copies.append(far_copy(n, j))
            pl.when(edge)(lambda: hop_copy(n).start())
            pl.when(jnp.logical_not(edge))(lambda: far_copy(n, j).start())

    def forward(n):
        @pl.when(jnp.logical_not(edge))
        def _():
            hop_copy(n).wait_recv()
            pass_copy(n).start()

    def near_copy(n):
        ys, zs = pl.ds(1, LY), pl.ds(0, LZ)
        return remote(t[n].at[near_plane, ys, zs, :], t[n].at[par * (LX + 1), ys, zs, :], n, NEAR, near)

    def y_copies(n, j):
        xs, zs = pl.ds(1 + x_half[j], HALF), pl.ds(0, LZ)
        r = t[n]
        return [remote(r.at[xs, LY, zs, :], r.at[xs, 0, zs, :], n, YLO + j, yup),
                remote(r.at[xs, 1, zs, :], r.at[xs, LY + 1, zs, :], n, YHI + j, ydn)]

    def z_copies(n, j):
        xs = pl.ds(x_half[j], HALF)
        return [remote(zsend.at[n, 0, xs], zrecv.at[n, 0, xs], n, ZLO + j, zup),
                remote(zsend.at[n, 1, xs], zrecv.at[n, 1, xs], n, ZHI + j, zdn)]

    def zpack(n, j):
        f = flat[n]
        for i in range(HALF):
            x = x_half[j] + i
            base = ((x + 1) * PY + 1) * PZ
            zsend[n, 0, x] = f[pl.ds(base + LZ - 1, LY, stride=PZ), :]
            zsend[n, 1, x] = f[pl.ds(base, LY, stride=PZ), :]

    def zunpack(n, j):
        f = flat[n]
        for i in range(HALF):
            x = x_half[j] + i
            base = ((x + 1) * PY + 1) * PZ
            f[pl.ds(base - 1, LY, stride=PZ), :] = zrecv[n, 0, x]
            f[pl.ds(base + LZ, LY, stride=PZ), :] = zrecv[n, 1, x]

    def columns(n, k, ys, sums):
        cur, nxt = flat[n], flat[n + 1]
        x = plane(k)
        for y in ys:
            base = pl.multiple_of(((x + 1) * PY + y + 1) * PZ, 8)
            wb = pl.multiple_of((x * LY + y) * LZ, 8)
            c = cur[pl.ds(base, LZ), :]
            beside = cur[pl.ds(base - PY * PZ, LZ), :] + cur[pl.ds(base + PY * PZ, LZ), :]
            beside = beside + (cur[pl.ds(base - PZ, LZ), :] + cur[pl.ds(base + PZ, LZ), :])
            beside = beside + (cur[pl.ds(base - 1, LZ), :] + cur[pl.ds(base + 1, LZ), :])
            new = w[pl.ds(wb, LZ), :] * c - (2.0 / 9.0) * beside
            if n == 0:
                new = 0.5 * new
                sums = (sums[0], sums[1], sums[2] + c * c)
            else:
                new = new - flat[n - 1][pl.ds(base, LZ), :]
            nxt[pl.ds(wb if n == ITERS - 1 else base, LZ), :] = new
            sums = (sums[0] + new * c, sums[1] + new * new, sums[2])
        return sums

    copies = []

    def send(cs):
        for c in cs:
            c.start()
            copies.append(c)

    def planes(n, lo, hi, ys, sums):
        return lax.fori_loop(lo, hi, lambda k, s: columns(n, k, ys, s), sums)

    send_far(0, 0)
    send_far(0, 1)
    send(y_copies(0, 0) + y_copies(0, 1) + [near_copy(0)])
    for j in range(2):
        zpack(0, j)
        send(z_copies(0, j))
    forward(0)

    def arrived(cs):
        for c in cs:
            c.wait_recv()

    rows = [None] * 9
    outer, inner = (0, LY - 1), range(1, LY - 1)
    for n in range(ITERS):
        more = n < ITERS - 1
        zero = jnp.zeros((LZ, R), jnp.float32)
        sums = (zero, zero, zero)
        arrived(z_copies(n, 0) + [near_copy(n)] + y_copies(n, 0))
        zunpack(n, 0)
        sums = planes(n, 0, HALF, outer, sums)
        if more:
            send(y_copies(n + 1, 0))
        sums = columns(n, 0, inner, sums)
        if more:
            send([near_copy(n + 1)])
        sums = planes(n, 1, HALF, inner, sums)
        if more:
            zpack(n + 1, 0)
            send(z_copies(n + 1, 0))
        arrived(z_copies(n, 1) + y_copies(n, 1))
        zunpack(n, 1)
        for j in range(2):
            arrived([far_copy(n, j)])
            sums = columns(n, LX - 1, range(j * LY // 2, (j + 1) * LY // 2), sums)
            if more:
                send_far(n + 1, j)
        sums = planes(n, HALF, LX - 1, outer, sums)
        if more:
            send(y_copies(n + 1, 1))
        sums = planes(n, HALF, LX - 1, inner, sums)
        if more:
            zpack(n + 1, 1)
            send(z_copies(n + 1, 1))
            forward(n + 1)
        if n == 0:
            rows[0] = jnp.sum(sums[2], axis=0, keepdims=True)
        rows[2 * n + 1] = jnp.sum(sums[0], axis=0, keepdims=True)
        rows[2 * n + 2] = jnp.sum(sums[1], axis=0, keepdims=True)

    def gather(peers, buf, mine, ssem, rsem):
        outs = []
        for i, peer in enumerate(peers):
            c = pltpu.make_async_remote_copy(
                src_ref=part, dst_ref=buf.at[mine], send_sem=ssem.at[i], recv_sem=rsem.at[mine],
                device_id=peer, device_id_type=MESH)
            c.start()
            outs.append(c)
        return outs

    def arrive(slots, peers, buf, rsem, ssem):
        for slot, peer in zip(slots, peers):
            pltpu.make_async_remote_copy(
                src_ref=part, dst_ref=buf.at[slot], send_sem=ssem.at[0], recv_sem=rsem.at[slot],
                device_id=peer, device_id_type=MESH).wait_recv()

    part[...] = jnp.concatenate(rows, axis=0)
    bufa[mine_a] = part[...]
    outs = gather(peers_a, bufa, mine_a, asend, arecv)
    arrive([lax.rem(row_y + i // 4, 4) * 4 + lax.rem(gz + i % 4, 4) for i in range(1, 16)], peers_a, bufa, arecv, asend)
    for c in outs:
        c.wait_send()
    total = bufa[0]
    for i in range(1, 16):
        total = total + bufa[i]
    part[...] = total
    bufb[mine_b] = total
    outs = gather(peers_b, bufb, mine_b, bsend, brecv)
    arrive([lax.rem(row_z + i // 4, 4) * 4 + lax.rem(gx + i % 4, 4) for i in range(1, 16)], peers_b, bufb, brecv, bsend)
    for c in outs:
        c.wait_send()
    total = bufb[0]
    for i in range(1, 16):
        total = total + bufb[i]
    order = lax.broadcasted_iota(jnp.int32, (9, R), 0)
    base = jnp.where(order % 2 == 0, total[0:1, :], total[1:2, :])
    mom_ref[...] = jnp.where(order < 2, total, 2.0 * total - base) * (1.0 / SITES)
    for c in copies:
        c.wait_send()

    @pl.when(jnp.logical_not(edge))
    def _():
        for n in range(ITERS):
            pass_copy(n).wait_send()


def shards(random_vectors, potential):
    padded = pltpu.VMEM((PX, PY, PZ, R), jnp.float32)
    dma = pltpu.SemaphoreType.DMA
    return pl.pallas_call(
        kernel,
        out_shape=(jax.ShapeDtypeStruct((9, R), jnp.float32),
                   jax.ShapeDtypeStruct((LX, LY, LZ, R), jnp.float32)),
        in_specs=[pl.BlockSpec(memory_space=pltpu.MemorySpace.HBM)] * 2,
        out_specs=(pl.BlockSpec(memory_space=pltpu.VMEM), pl.BlockSpec(memory_space=pltpu.VMEM)),
        scratch_shapes=[padded] * 4 + [
            pltpu.VMEM((LX * LY * LZ, R), jnp.float32),
            pltpu.VMEM((LX, LY, LZ), jnp.float32),
            pltpu.VMEM((ITERS, 2, LX, LY, R), jnp.float32),
            pltpu.VMEM((ITERS, 2, LX, LY, R), jnp.float32),
            pltpu.VMEM((ITERS, LY // 2, LZ, R), jnp.float32),
            pltpu.VMEM((9, R), jnp.float32),
            pltpu.VMEM((16, 9, R), jnp.float32),
            pltpu.VMEM((16, 9, R), jnp.float32),
            dma, dma, dma((ITERS, WAYS)), dma((ITERS, WAYS)), dma((ITERS,)), dma((ITERS,)),
            dma((16,)), dma((16,)), dma((16,)), dma((16,)),
        ],
        compiler_params=pltpu.CompilerParams(
            collective_id=0, has_side_effects=True, vmem_limit_bytes=48 * 1024 * 1024),
    )(random_vectors, potential)


def solution(mesh):
    placed = (P("gx", "gy", "gz", None), P("gx", "gy", "gz"))
    return jax.shard_map(
        shards, mesh=mesh, in_specs=placed, out_specs=(P(), P("gx", "gy", "gz", None)), check_vma=False)
```

```python
import jax
import jax.numpy as jnp
from jax import lax
from jax.experimental import pallas as pl
from jax.experimental.pallas import tpu as pltpu
from jax.sharding import PartitionSpec as P

LX, LY, LZ, R = 16, 8, 32, 128
ITERS = 4
PX, PY, PZ = LX + 1 + ITERS, LY + 2, 40
CUTS = (0, LX // 2, LX - 1)
SITES = 64 * 128 * 128
MESH = pl.DeviceIdType.MESH
COPIES = 88
LIMIT = 48 * 1024 * 1024


def kernel(v_ref, pot_ref, mom_ref, out_ref, t0, t1, t2, t3, w, pot, pot_halo, zsend, zrecv, dsend, drecv, relay,
           part, bufa, bufb, load_sem, pot_sem, send_sem, recv_sem, asend, arecv, bsend, brecv):
    gx, gy, gz = lax.axis_index("gx"), lax.axis_index("gy"), lax.axis_index("gz")
    t = [t0, t1, t2, t3]
    flat = [r.reshape(PX * PY * PZ, R) for r in t] + [out_ref.reshape(LX * LY * LZ, R)]
    par = lax.rem(gx, 2)
    row_y = lax.rem(gy, 4)
    row_z = gy // 4

    def plane(k):
        return k * par + (LX - 1 - k) * (1 - par)

    loads = [pltpu.make_async_copy(v_ref.at[plane(k)], t0.at[k + 1, pl.ds(1, LY), pl.ds(0, LZ), :], load_sem.at[k])
             for k in range(LX)]
    for c in loads:
        c.start()
    load_pot = pltpu.make_async_copy(pot_ref, pot, pot_sem)
    load_pot.start()

    mine_a = row_y * 4 + gz
    mine_b = row_z * 4 + gx
    peers_a = [(gx, row_z * 4 + lax.rem(row_y + i // 4, 4), lax.rem(gz + i % 4, 4)) for i in range(1, 16)]
    peers_b = [(lax.rem(gx + i % 4, 4), lax.rem(row_z + i // 4, 4) * 4 + row_y, gz) for i in range(1, 16)]
    far = (lax.rem(gx + 2 * par + 3, 4), gy, gz)
    near = (gx + 1 - 2 * par, gy, gz)
    ydn, yup = (gx, lax.rem(gy + 15, 16), gz), (gx, lax.rem(gy + 1, 16), gz)
    zdn, zup = (gx, gy, lax.rem(gz + 3, 4)), (gx, gy, lax.rem(gz + 1, 4))
    barrier = pltpu.get_barrier_semaphore()
    side = 1 - 2 * lax.rem(row_y, 2)
    edge = (row_y == 0) | (row_y == 3)
    beside = (gx, gy + side, gz)
    diag = (far[0], gy + side, gz)
    greeted = [far, near, ydn, yup, zdn, zup, diag] + peers_a + peers_b
    for peer in greeted:
        pl.semaphore_signal(barrier, inc=1, device_id=peer, device_id_type=MESH)

    load_pot.wait()
    for c in loads:
        c.wait()
    pl.semaphore_wait(barrier, len(greeted))

    index = {}

    def remote(key, src, dst, peer):
        i = index.setdefault(key, len(index))
        return pltpu.make_async_remote_copy(
            src_ref=src, dst_ref=dst, send_sem=send_sem.at[i], recv_sem=recv_sem.at[i],
            device_id=peer, device_id_type=MESH)

    rows_z = pl.ds(0, LZ)
    halves = [pl.ds(1, LY // 2), pl.ds(1 + LY // 2, LY // 2)]

    def far_copy(p, j):
        return remote(("far", p, j), t0.at[LX - p, halves[j], rows_z, :], t0.at[LX + 1 + p, halves[j], rows_z, :], far)

    def hop_copy(p):
        return remote(("hop", p), t0.at[LX - p, halves[1], rows_z, :], relay.at[p], beside)

    def pass_copy(p):
        i, k = index.setdefault(("pass", p), len(index)), index[("far", p, 1)]
        return pltpu.make_async_remote_copy(
            src_ref=relay.at[p], dst_ref=t0.at[LX + 1 + p, halves[1], rows_z, :],
            send_sem=send_sem.at[i], recv_sem=recv_sem.at[k], device_id=diag, device_id_type=MESH)

    def near_copy(n):
        return remote(("near", n), t[n].at[1, pl.ds(1, LY), rows_z, :], t[n].at[0, pl.ds(1, LY), rows_z, :], near)

    def y_pair(name, n, ks):
        r = t[n]
        return [remote(name + ("lo",), r.at[ks, LY, rows_z, :], r.at[ks, 0, rows_z, :], yup),
                remote(name + ("hi",), r.at[ks, 1, rows_z, :], r.at[ks, LY + 1, rows_z, :], ydn)]

    def y_copies(n, j):
        return y_pair(("y", n, j), n, pl.ds(1 + CUTS[j], CUTS[j + 1] - CUTS[j]))

    def z_copies(n, j):
        ks = pl.ds(CUTS[j], CUTS[j + 1] - CUTS[j])
        return [remote(("z", n, j, "lo"), zsend.at[n, 0, ks], zrecv.at[n, 0, ks], zup),
                remote(("z", n, j, "hi"), zsend.at[n, 1, ks], zrecv.at[n, 1, ks], zdn)]

    def skew(p):
        return [(m, LX - 1 + p - m) for m in range(p + 1)]

    def skew_y(p):
        return [c for m, k in skew(p) for c in y_pair(("dy", p, m), m, k + 1)]

    def skew_z(p):
        ms = pl.ds(0, p + 1)
        return [remote(("dz", p, "lo"), dsend.at[p, 0, ms], drecv.at[p, 0, ms], zup),
                remote(("dz", p, "hi"), dsend.at[p, 1, ms], drecv.at[p, 1, ms], zdn)]

    def pot_copy(i):
        return remote(("pot", i), pot.at[plane(LX - 1 - i)], pot_halo.at[i], far)

    def ends(n, k):
        base = ((k + 1) * PY + 1) * PZ
        return flat[n][pl.ds(base + LZ - 1, LY, stride=PZ), :], flat[n][pl.ds(base, LY, stride=PZ), :]

    def set_ends(n, k, lo, hi):
        base = ((k + 1) * PY + 1) * PZ
        flat[n][pl.ds(base - 1, LY, stride=PZ), :] = lo
        flat[n][pl.ds(base + LZ, LY, stride=PZ), :] = hi

    def zpack(n, j):
        for k in range(CUTS[j], CUTS[j + 1]):
            zsend[n, 0, k], zsend[n, 1, k] = ends(n, k)

    def zunpack(n, j):
        for k in range(CUTS[j], CUTS[j + 1]):
            set_ends(n, k, zrecv[n, 0, k], zrecv[n, 1, k])

    def skew_pack(p):
        for m, k in skew(p):
            dsend[p, 0, m], dsend[p, 1, m] = ends(m, k)

    def skew_unpack(p):
        for m, k in skew(p):
            set_ends(m, k, drecv[p, 0, m], drecv[p, 1, m])

    def columns(n, k, ys, sums):
        cur, nxt = flat[n], flat[n + 1]
        for y in ys:
            base = pl.multiple_of(((k + 1) * PY + y + 1) * PZ, 8)
            c = cur[pl.ds(base, LZ), :]
            beside = cur[pl.ds(base - PY * PZ, LZ), :] + cur[pl.ds(base + PY * PZ, LZ), :]
            beside = beside + (cur[pl.ds(base - PZ, LZ), :] + cur[pl.ds(base + PZ, LZ), :])
            beside = beside + (cur[pl.ds(base - 1, LZ), :] + cur[pl.ds(base + 1, LZ), :])
            new = w[pl.ds(pl.multiple_of((k * LY + y) * LZ, 8), LZ), :] * c - (2.0 / 9.0) * beside
            if n == 0:
                new = 0.5 * new
            else:
                new = new - flat[n - 1][pl.ds(base, LZ), :]
            if n == ITERS - 1:
                nxt[pl.ds(pl.multiple_of((plane(k) * LY + y) * LZ, 8), LZ), :] = new
            else:
                nxt[pl.ds(base, LZ), :] = new
            if sums is not None:
                sums = (sums[0] + new * c, sums[1] + new * new, sums[2] + c * c if n == 0 else sums[2])
        return sums

    copies = []

    def send(cs):
        for c in cs:
            c.start()
            copies.append(c)

    def planes(n, lo, hi, ys, sums):
        return lax.fori_loop(lo, hi, lambda k, s: columns(n, k, ys, s), sums)

    def send_far(p):
        send([far_copy(p, 0)])
        direct = far_copy(p, 1)
        hop = hop_copy(p)

        @pl.when(edge)
        def _():
            hop.start()

        @pl.when(jnp.logical_not(edge))
        def _():
            direct.start()

    def forward(p):
        @pl.when(jnp.logical_not(edge))
        def _():
            hop_copy(p).wait_recv()
            pass_copy(p).start()

    def arrived(cs):
        for c in cs:
            c.wait_recv()

    send_far(0)
    for j in range(2):
        send(y_copies(0, j))
    send(skew_y(0) + [near_copy(0)])
    for j in range(2):
        zpack(0, j)
        send(z_copies(0, j))
    skew_pack(0)
    send(skew_z(0) + [pot_copy(i) for i in range(ITERS - 1)])
    send_far(1)

    pot_t = jnp.transpose(pot[...].reshape(LX * LY, LZ)) * (2.0 / 9.0)
    for x in range(LX):
        for y in range(LY):
            start = pl.multiple_of((plane(x) * LY + y) * LZ, 8)
            w[pl.ds(start, LZ), :] = jnp.broadcast_to(pot_t[:, x * LY + y:x * LY + y + 1], (LZ, R))
    forward(0)

    rows = [None] * 9
    outer, inner = (0, LY - 1), range(1, LY - 1)
    for n in range(ITERS):
        more = n < ITERS - 1
        zero = jnp.zeros((LZ, R), jnp.float32)
        sums = (zero, zero, zero)
        arrived(z_copies(n, 0) + [near_copy(n)] + y_copies(n, 0))
        zunpack(n, 0)
        sums = planes(n, CUTS[0], CUTS[1], outer, sums)
        if more:
            send(y_copies(n + 1, 0))
        arrived(z_copies(n, 1) + y_copies(n, 1))
        zunpack(n, 1)
        sums = planes(n, CUTS[1], CUTS[2], outer, sums)
        if more:
            send(y_copies(n + 1, 1))
        if n + 2 < ITERS:
            send_far(n + 2)
        if more:
            forward(n + 1)
        sums = columns(n, 0, inner, sums)
        if more:
            send([near_copy(n + 1)])
        sums = planes(n, 1, CUTS[1], inner, sums)
        if more:
            zpack(n + 1, 0)
            send(z_copies(n + 1, 0))
        sums = planes(n, CUTS[1], CUTS[2], inner, sums)
        if more:
            zpack(n + 1, 1)
            send(z_copies(n + 1, 1))
        if n == 1:
            arrived([pot_copy(i) for i in range(ITERS - 1)])
            halo_t = jnp.transpose(pot_halo[...].reshape((ITERS - 1) * LY, LZ)) * (2.0 / 9.0)
            for i in range((ITERS - 1) * LY):
                start = (LX * LY + i) * LZ
                w[start:start + LZ, :] = jnp.broadcast_to(halo_t[:, i:i + 1], (LZ, R))
        arrived(skew_z(n) + skew_y(n))
        skew_unpack(n)
        arrived([far_copy(n, 0), far_copy(n, 1)])
        for m, k in skew(n):
            if m < n:
                columns(m, k, range(LY), None)
            else:
                sums = columns(m, k, range(LY), sums)
        if more:
            send(skew_y(n + 1))
            skew_pack(n + 1)
            send(skew_z(n + 1))
        if n == 0:
            rows[0] = jnp.sum(sums[2], axis=0, keepdims=True)
        rows[2 * n + 1] = jnp.sum(sums[0], axis=0, keepdims=True)
        rows[2 * n + 2] = jnp.sum(sums[1], axis=0, keepdims=True)

    def gather(peers, buf, mine, ssem, rsem):
        outs = []
        for i, peer in enumerate(peers):
            c = pltpu.make_async_remote_copy(
                src_ref=part, dst_ref=buf.at[mine], send_sem=ssem.at[i], recv_sem=rsem.at[mine],
                device_id=peer, device_id_type=MESH)
            c.start()
            outs.append(c)
        return outs

    def arrive(slots, peers, buf, rsem, ssem):
        for slot, peer in zip(slots, peers):
            pltpu.make_async_remote_copy(
                src_ref=part, dst_ref=buf.at[slot], send_sem=ssem.at[0], recv_sem=rsem.at[slot],
                device_id=peer, device_id_type=MESH).wait_recv()

    part[...] = jnp.concatenate(rows, axis=0)
    bufa[mine_a] = part[...]
    outs = gather(peers_a, bufa, mine_a, asend, arecv)
    arrive([lax.rem(row_y + i // 4, 4) * 4 + lax.rem(gz + i % 4, 4) for i in range(1, 16)], peers_a, bufa, arecv, asend)
    for c in outs:
        c.wait_send()
    total = bufa[0]
    for i in range(1, 16):
        total = total + bufa[i]
    part[...] = total
    bufb[mine_b] = total
    outs = gather(peers_b, bufb, mine_b, bsend, brecv)
    arrive([lax.rem(row_z + i // 4, 4) * 4 + lax.rem(gx + i % 4, 4) for i in range(1, 16)], peers_b, bufb, brecv, bsend)
    for c in outs:
        c.wait_send()
    total = bufb[0]
    for i in range(1, 16):
        total = total + bufb[i]
    order = lax.broadcasted_iota(jnp.int32, (9, R), 0)
    base = jnp.where(order % 2 == 0, total[0:1, :], total[1:2, :])
    mom_ref[...] = jnp.where(order < 2, total, 2.0 * total - base) * (1.0 / SITES)
    for c in copies:
        c.wait_send()

    @pl.when(edge)
    def _():
        for p in range(ITERS):
            hop_copy(p).wait_send()

    @pl.when(jnp.logical_not(edge))
    def _():
        for p in range(ITERS):
            far_copy(p, 1).wait_send()
            pass_copy(p).wait_send()


def shards(random_vectors, potential):
    padded = pltpu.VMEM((PX, PY, PZ, R), jnp.float32)
    dma = pltpu.SemaphoreType.DMA
    return pl.pallas_call(
        kernel,
        out_shape=(jax.ShapeDtypeStruct((9, R), jnp.float32),
                   jax.ShapeDtypeStruct((LX, LY, LZ, R), jnp.float32)),
        in_specs=[pl.BlockSpec(memory_space=pltpu.MemorySpace.HBM)] * 2,
        out_specs=(pl.BlockSpec(memory_space=pltpu.VMEM), pl.BlockSpec(memory_space=pltpu.VMEM)),
        scratch_shapes=[padded] * 4 + [
            pltpu.VMEM(((LX + ITERS - 1) * LY * LZ, R), jnp.float32),
            pltpu.VMEM((LX, LY, LZ), jnp.float32),
            pltpu.VMEM((ITERS - 1, LY, LZ), jnp.float32),
            pltpu.VMEM((ITERS, 2, LX, LY, R), jnp.float32),
            pltpu.VMEM((ITERS, 2, LX, LY, R), jnp.float32),
            pltpu.VMEM((ITERS, 2, ITERS, LY, R), jnp.float32),
            pltpu.VMEM((ITERS, 2, ITERS, LY, R), jnp.float32),
            pltpu.VMEM((ITERS, LY // 2, LZ, R), jnp.float32),
            pltpu.VMEM((9, R), jnp.float32),
            pltpu.VMEM((16, 9, R), jnp.float32),
            pltpu.VMEM((16, 9, R), jnp.float32),
            dma((LX,)), dma, dma((COPIES,)), dma((COPIES,)),
            dma((16,)), dma((16,)), dma((16,)), dma((16,)),
        ],
        compiler_params=pltpu.CompilerParams(
            collective_id=0, has_side_effects=True, vmem_limit_bytes=LIMIT),
    )(pltpu.with_memory_space_constraint(random_vectors, pltpu.HBM), pltpu.with_memory_space_constraint(potential, pltpu.HBM))


def solution(mesh):
    placed = (P("gx", "gy", "gz", None), P("gx", "gy", "gz"))
    return jax.shard_map(
        shards, mesh=mesh, in_specs=placed, out_specs=(P(), P("gx", "gy", "gz", None)), check_vma=False)
```

```python
import jax
import jax.numpy as jnp
from jax import lax
from jax.experimental import pallas as pl
from jax.experimental.pallas import tpu as pltpu
from jax.sharding import PartitionSpec as P

LX, LY, LZ, R = 16, 8, 32, 128
ITERS = 4
PX, PY, PZ = LX + 1 + ITERS, LY + 2, 40
CUTS = (0, LX // 2, LX - 1)
SITES = 64 * 128 * 128
MESH = pl.DeviceIdType.MESH
COPIES = 88
LIMIT = 48 * 1024 * 1024


def kernel(v_ref, pot_ref, mom_ref, out_ref, t0, t1, t2, t3, w, pot, pot_halo, zsend, zrecv, dsend, drecv, relay,
           part, bufa, bufb, load_sem, pot_sem, send_sem, recv_sem, asend, arecv, bsend, brecv):
    gx, gy, gz = lax.axis_index("gx"), lax.axis_index("gy"), lax.axis_index("gz")
    t = [t0, t1, t2, t3]
    flat = [r.reshape(PX * PY * PZ, R) for r in t] + [out_ref.reshape(LX * LY * LZ, R)]
    par = lax.rem(gx, 2)
    row_y = lax.rem(gy, 4)
    row_z = gy // 4

    def plane(k):
        return k * par + (LX - 1 - k) * (1 - par)

    loads = [pltpu.make_async_copy(v_ref.at[plane(k)], t0.at[k + 1, pl.ds(1, LY), pl.ds(0, LZ), :], load_sem.at[k])
             for k in range(LX)]
    for c in loads:
        c.start()
    load_pot = pltpu.make_async_copy(pot_ref, pot, pot_sem)
    load_pot.start()

    mine_a = row_y * 4 + gz
    mine_b = row_z * 4 + gx
    peers_a = [(gx, row_z * 4 + lax.rem(row_y + i // 4, 4), lax.rem(gz + i % 4, 4)) for i in range(1, 16)]
    peers_b = [(lax.rem(gx + i % 4, 4), lax.rem(row_z + i // 4, 4) * 4 + row_y, gz) for i in range(1, 16)]
    far = (lax.rem(gx + 2 * par + 3, 4), gy, gz)
    near = (gx + 1 - 2 * par, gy, gz)
    ydn, yup = (gx, lax.rem(gy + 15, 16), gz), (gx, lax.rem(gy + 1, 16), gz)
    zdn, zup = (gx, gy, lax.rem(gz + 3, 4)), (gx, gy, lax.rem(gz + 1, 4))
    barrier = pltpu.get_barrier_semaphore()
    side = 1 - 2 * lax.rem(row_y, 2)
    edge = (row_y == 0) | (row_y == 3)
    beside = (gx, gy + side, gz)
    diag = (far[0], gy + side, gz)
    greeted = [far, near, ydn, yup, zdn, zup, diag] + peers_a + peers_b
    for peer in greeted:
        pl.semaphore_signal(barrier, inc=1, device_id=peer, device_id_type=MESH)

    load_pot.wait()
    for c in loads:
        c.wait()
    pl.semaphore_wait(barrier, len(greeted))

    index = {}

    def remote(key, src, dst, peer):
        i = index.setdefault(key, len(index))
        return pltpu.make_async_remote_copy(
            src_ref=src, dst_ref=dst, send_sem=send_sem.at[i], recv_sem=recv_sem.at[i],
            device_id=peer, device_id_type=MESH)

    rows_z = pl.ds(0, LZ)
    halves = [pl.ds(1, LY // 2), pl.ds(1 + LY // 2, LY // 2)]

    def far_copy(p, j):
        return remote(("far", p, j), t0.at[LX - p, halves[j], rows_z, :], t0.at[LX + 1 + p, halves[j], rows_z, :], far)

    def hop_copy(p):
        return remote(("hop", p), t0.at[LX - p, halves[1], rows_z, :], relay.at[p], beside)

    def pass_copy(p):
        i, k = index.setdefault(("pass", p), len(index)), index[("far", p, 1)]
        return pltpu.make_async_remote_copy(
            src_ref=relay.at[p], dst_ref=t0.at[LX + 1 + p, halves[1], rows_z, :],
            send_sem=send_sem.at[i], recv_sem=recv_sem.at[k], device_id=diag, device_id_type=MESH)

    def near_copy(n):
        return remote(("near", n), t[n].at[1, pl.ds(1, LY), rows_z, :], t[n].at[0, pl.ds(1, LY), rows_z, :], near)

    def y_pair(name, n, ks):
        r = t[n]
        return [remote(name + ("lo",), r.at[ks, LY, rows_z, :], r.at[ks, 0, rows_z, :], yup),
                remote(name + ("hi",), r.at[ks, 1, rows_z, :], r.at[ks, LY + 1, rows_z, :], ydn)]

    def y_copies(n, j):
        return y_pair(("y", n, j), n, pl.ds(1 + CUTS[j], CUTS[j + 1] - CUTS[j]))

    def z_copies(n, j):
        ks = pl.ds(CUTS[j], CUTS[j + 1] - CUTS[j])
        return [remote(("z", n, j, "lo"), zsend.at[n, 0, ks], zrecv.at[n, 0, ks], zup),
                remote(("z", n, j, "hi"), zsend.at[n, 1, ks], zrecv.at[n, 1, ks], zdn)]

    def skew(p):
        return [(m, LX - 1 + p - m) for m in range(p + 1)]

    def skew_y(p):
        return [c for m, k in skew(p) for c in y_pair(("dy", p, m), m, k + 1)]

    def skew_z(p):
        ms = pl.ds(0, p + 1)
        return [remote(("dz", p, "lo"), dsend.at[p, 0, ms], drecv.at[p, 0, ms], zup),
                remote(("dz", p, "hi"), dsend.at[p, 1, ms], drecv.at[p, 1, ms], zdn)]

    def pot_copy(i):
        return remote(("pot", i), pot.at[plane(LX - 1 - i)], pot_halo.at[i], far)

    def ends(n, k):
        base = ((k + 1) * PY + 1) * PZ
        return flat[n][pl.ds(base + LZ - 1, LY, stride=PZ), :], flat[n][pl.ds(base, LY, stride=PZ), :]

    def set_ends(n, k, lo, hi):
        base = ((k + 1) * PY + 1) * PZ
        flat[n][pl.ds(base - 1, LY, stride=PZ), :] = lo
        flat[n][pl.ds(base + LZ, LY, stride=PZ), :] = hi

    def zpack(n, j):
        for k in range(CUTS[j], CUTS[j + 1]):
            zsend[n, 0, k], zsend[n, 1, k] = ends(n, k)

    def zunpack(n, j):
        for k in range(CUTS[j], CUTS[j + 1]):
            set_ends(n, k, zrecv[n, 0, k], zrecv[n, 1, k])

    def skew_pack(p):
        for m, k in skew(p):
            dsend[p, 0, m], dsend[p, 1, m] = ends(m, k)

    def skew_unpack(p):
        for m, k in skew(p):
            set_ends(m, k, drecv[p, 0, m], drecv[p, 1, m])

    def columns(n, k, ys, sums):
        cur, nxt = flat[n], flat[n + 1]
        for y in ys:
            base = pl.multiple_of(((k + 1) * PY + y + 1) * PZ, 8)
            c = cur[pl.ds(base, LZ), :]
            beside = cur[pl.ds(base - PY * PZ, LZ), :] + cur[pl.ds(base + PY * PZ, LZ), :]
            beside = beside + (cur[pl.ds(base - PZ, LZ), :] + cur[pl.ds(base + PZ, LZ), :])
            beside = beside + (cur[pl.ds(base - 1, LZ), :] + cur[pl.ds(base + 1, LZ), :])
            new = w[pl.ds(pl.multiple_of((k * LY + y) * LZ, 8), LZ), :] * c - (2.0 / 9.0) * beside
            if n == 0:
                new = 0.5 * new
            else:
                new = new - flat[n - 1][pl.ds(base, LZ), :]
            if n == ITERS - 1:
                nxt[pl.ds(pl.multiple_of((plane(k) * LY + y) * LZ, 8), LZ), :] = new
            else:
                nxt[pl.ds(base, LZ), :] = new
            if sums is not None:
                sums = (sums[0] + new * c, sums[1] + new * new, sums[2] + c * c if n == 0 else sums[2])
        return sums

    copies = []

    def send(cs):
        for c in cs:
            c.start()
            copies.append(c)

    def planes(n, lo, hi, ys, sums):
        return lax.fori_loop(lo, hi, lambda k, s: columns(n, k, ys, s), sums)

    def send_far(p):
        send([far_copy(p, 0)])
        direct = far_copy(p, 1)
        hop = hop_copy(p)

        @pl.when(edge)
        def _():
            hop.start()

        @pl.when(jnp.logical_not(edge))
        def _():
            direct.start()

    def forward(p):
        @pl.when(jnp.logical_not(edge))
        def _():
            hop_copy(p).wait_recv()
            pass_copy(p).start()

    def arrived(cs):
        for c in cs:
            c.wait_recv()

    send_far(0)
    for j in range(2):
        send(y_copies(0, j))
    send(skew_y(0) + [near_copy(0)])
    for j in range(2):
        zpack(0, j)
        send(z_copies(0, j))
    skew_pack(0)
    send(skew_z(0) + [pot_copy(i) for i in range(ITERS - 1)])

    pot_t = jnp.transpose(pot[...].reshape(LX * LY, LZ)) * (2.0 / 9.0)
    for x in range(LX):
        for y in range(LY):
            start = pl.multiple_of((plane(x) * LY + y) * LZ, 8)
            w[pl.ds(start, LZ), :] = jnp.broadcast_to(pot_t[:, x * LY + y:x * LY + y + 1], (LZ, R))
    forward(0)

    rows = [None] * 9
    outer, inner = (0, LY - 1), range(1, LY - 1)
    for n in range(ITERS):
        more = n < ITERS - 1
        zero = jnp.zeros((LZ, R), jnp.float32)
        sums = (zero, zero, zero)
        arrived(z_copies(n, 0) + [near_copy(n)] + y_copies(n, 0))
        zunpack(n, 0)
        sums = planes(n, CUTS[0], CUTS[1], outer, sums)
        if more:
            send(y_copies(n + 1, 0))
            send_far(n + 1)
        arrived(z_copies(n, 1) + y_copies(n, 1))
        zunpack(n, 1)
        sums = planes(n, CUTS[1], CUTS[2], outer, sums)
        if more:
            send(y_copies(n + 1, 1))
        sums = columns(n, 0, inner, sums)
        if more:
            send([near_copy(n + 1)])
        sums = planes(n, 1, CUTS[1], inner, sums)
        if more:
            zpack(n + 1, 0)
            send(z_copies(n + 1, 0))
        sums = planes(n, CUTS[1], CUTS[2], inner, sums)
        if more:
            zpack(n + 1, 1)
            send(z_copies(n + 1, 1))
        if n == 1:
            arrived([pot_copy(i) for i in range(ITERS - 1)])
            halo_t = jnp.transpose(pot_halo[...].reshape((ITERS - 1) * LY, LZ)) * (2.0 / 9.0)
            for i in range((ITERS - 1) * LY):
                start = (LX * LY + i) * LZ
                w[start:start + LZ, :] = jnp.broadcast_to(halo_t[:, i:i + 1], (LZ, R))
        if more:
            forward(n + 1)
        arrived(skew_z(n) + skew_y(n))
        skew_unpack(n)
        arrived([far_copy(n, 0), far_copy(n, 1)])
        for m, k in skew(n):
            if m < n:
                columns(m, k, range(LY), None)
            else:
                sums = columns(m, k, range(LY), sums)
        if more:
            send(skew_y(n + 1))
            skew_pack(n + 1)
            send(skew_z(n + 1))
        if n == 0:
            rows[0] = jnp.sum(sums[2], axis=0, keepdims=True)
        rows[2 * n + 1] = jnp.sum(sums[0], axis=0, keepdims=True)
        rows[2 * n + 2] = jnp.sum(sums[1], axis=0, keepdims=True)

    def gather(peers, buf, mine, ssem, rsem):
        outs = []
        for i, peer in enumerate(peers):
            c = pltpu.make_async_remote_copy(
                src_ref=part, dst_ref=buf.at[mine], send_sem=ssem.at[i], recv_sem=rsem.at[mine],
                device_id=peer, device_id_type=MESH)
            c.start()
            outs.append(c)
        return outs

    def arrive(slots, peers, buf, rsem, ssem):
        for slot, peer in zip(slots, peers):
            pltpu.make_async_remote_copy(
                src_ref=part, dst_ref=buf.at[slot], send_sem=ssem.at[0], recv_sem=rsem.at[slot],
                device_id=peer, device_id_type=MESH).wait_recv()

    part[...] = jnp.concatenate(rows, axis=0)
    bufa[mine_a] = part[...]
    outs = gather(peers_a, bufa, mine_a, asend, arecv)
    arrive([lax.rem(row_y + i // 4, 4) * 4 + lax.rem(gz + i % 4, 4) for i in range(1, 16)], peers_a, bufa, arecv, asend)
    for c in outs:
        c.wait_send()
    total = bufa[0]
    for i in range(1, 16):
        total = total + bufa[i]
    part[...] = total
    bufb[mine_b] = total
    outs = gather(peers_b, bufb, mine_b, bsend, brecv)
    arrive([lax.rem(row_z + i // 4, 4) * 4 + lax.rem(gx + i % 4, 4) for i in range(1, 16)], peers_b, bufb, brecv, bsend)
    for c in outs:
        c.wait_send()
    total = bufb[0]
    for i in range(1, 16):
        total = total + bufb[i]
    order = lax.broadcasted_iota(jnp.int32, (9, R), 0)
    base = jnp.where(order % 2 == 0, total[0:1, :], total[1:2, :])
    mom_ref[...] = jnp.where(order < 2, total, 2.0 * total - base) * (1.0 / SITES)
    for c in copies:
        c.wait_send()

    @pl.when(edge)
    def _():
        for p in range(ITERS):
            hop_copy(p).wait_send()

    @pl.when(jnp.logical_not(edge))
    def _():
        for p in range(ITERS):
            far_copy(p, 1).wait_send()
            pass_copy(p).wait_send()


def shards(random_vectors, potential):
    padded = pltpu.VMEM((PX, PY, PZ, R), jnp.float32)
    dma = pltpu.SemaphoreType.DMA
    return pl.pallas_call(
        kernel,
        out_shape=(jax.ShapeDtypeStruct((9, R), jnp.float32),
                   jax.ShapeDtypeStruct((LX, LY, LZ, R), jnp.float32)),
        in_specs=[pl.BlockSpec(memory_space=pltpu.MemorySpace.HBM)] * 2,
        out_specs=(pl.BlockSpec(memory_space=pltpu.VMEM), pl.BlockSpec(memory_space=pltpu.VMEM)),
        scratch_shapes=[padded] * 4 + [
            pltpu.VMEM(((LX + ITERS - 1) * LY * LZ, R), jnp.float32),
            pltpu.VMEM((LX, LY, LZ), jnp.float32),
            pltpu.VMEM((ITERS - 1, LY, LZ), jnp.float32),
            pltpu.VMEM((ITERS, 2, LX, LY, R), jnp.float32),
            pltpu.VMEM((ITERS, 2, LX, LY, R), jnp.float32),
            pltpu.VMEM((ITERS, 2, ITERS, LY, R), jnp.float32),
            pltpu.VMEM((ITERS, 2, ITERS, LY, R), jnp.float32),
            pltpu.VMEM((ITERS, LY // 2, LZ, R), jnp.float32),
            pltpu.VMEM((9, R), jnp.float32),
            pltpu.VMEM((16, 9, R), jnp.float32),
            pltpu.VMEM((16, 9, R), jnp.float32),
            dma((LX,)), dma, dma((COPIES,)), dma((COPIES,)),
            dma((16,)), dma((16,)), dma((16,)), dma((16,)),
        ],
        compiler_params=pltpu.CompilerParams(
            collective_id=0, has_side_effects=True, vmem_limit_bytes=LIMIT),
    )(pltpu.with_memory_space_constraint(random_vectors, pltpu.HBM), pltpu.with_memory_space_constraint(potential, pltpu.HBM))


def solution(mesh):
    placed = (P("gx", "gy", "gz", None), P("gx", "gy", "gz"))
    return jax.shard_map(
        shards, mesh=mesh, in_specs=placed, out_specs=(P(), P("gx", "gy", "gz", None)), check_vma=False)
```

```python
import jax
import jax.numpy as jnp
from jax import lax
from jax.experimental import pallas as pl
from jax.experimental.pallas import tpu as pltpu
from jax.sharding import PartitionSpec as P

LX, LY, LZ, R = 16, 8, 32, 128
ITERS = 4
PX, PY, PZ = LX + 1 + ITERS, LY + 2, 40
CUTS = (0, 9, LX - 1)
SITES = 64 * 128 * 128
MESH = pl.DeviceIdType.MESH
COPIES = 88
LIMIT = 48 * 1024 * 1024


def kernel(v_ref, pot_ref, mom_ref, out_ref, t0, t1, t2, t3, w, pot, pot_halo, zsend, zrecv, dsend, drecv, relay,
           part, bufa, bufb, load_sem, pot_sem, send_sem, recv_sem, asend, arecv, bsend, brecv):
    gx, gy, gz = lax.axis_index("gx"), lax.axis_index("gy"), lax.axis_index("gz")
    t = [t0, t1, t2, t3]
    flat = [r.reshape(PX * PY * PZ, R) for r in t] + [out_ref.reshape(LX * LY * LZ, R)]
    par = lax.rem(gx, 2)
    row_y = lax.rem(gy, 4)
    row_z = gy // 4

    def plane(k):
        return k * par + (LX - 1 - k) * (1 - par)

    loads = [pltpu.make_async_copy(v_ref.at[plane(k)], t0.at[k + 1, pl.ds(1, LY), pl.ds(0, LZ), :], load_sem.at[k])
             for k in range(LX)]
    for c in loads:
        c.start()
    load_pot = pltpu.make_async_copy(pot_ref, pot, pot_sem)
    load_pot.start()

    mine_a = row_y * 4 + gz
    mine_b = row_z * 4 + gx
    peers_a = [(gx, row_z * 4 + lax.rem(row_y + i // 4, 4), lax.rem(gz + i % 4, 4)) for i in range(1, 16)]
    peers_b = [(lax.rem(gx + i % 4, 4), lax.rem(row_z + i // 4, 4) * 4 + row_y, gz) for i in range(1, 16)]
    far = (lax.rem(gx + 2 * par + 3, 4), gy, gz)
    near = (gx + 1 - 2 * par, gy, gz)
    ydn, yup = (gx, lax.rem(gy + 15, 16), gz), (gx, lax.rem(gy + 1, 16), gz)
    zdn, zup = (gx, gy, lax.rem(gz + 3, 4)), (gx, gy, lax.rem(gz + 1, 4))
    barrier = pltpu.get_barrier_semaphore()
    side = 1 - 2 * lax.rem(row_y, 2)
    edge = (row_y == 0) | (row_y == 3)
    beside = (gx, gy + side, gz)
    diag = (far[0], gy + side, gz)
    greeted = [far, near, ydn, yup, zdn, zup, diag] + peers_a + peers_b
    for peer in greeted:
        pl.semaphore_signal(barrier, inc=1, device_id=peer, device_id_type=MESH)

    load_pot.wait()
    for c in loads:
        c.wait()
    pl.semaphore_wait(barrier, len(greeted))

    index = {}

    def remote(key, src, dst, peer):
        i = index.setdefault(key, len(index))
        return pltpu.make_async_remote_copy(
            src_ref=src, dst_ref=dst, send_sem=send_sem.at[i], recv_sem=recv_sem.at[i],
            device_id=peer, device_id_type=MESH)

    rows_z = pl.ds(0, LZ)
    halves = [pl.ds(1, LY // 2), pl.ds(1 + LY // 2, LY // 2)]

    def far_copy(p, j):
        return remote(("far", p, j), t0.at[LX - p, halves[j], rows_z, :], t0.at[LX + 1 + p, halves[j], rows_z, :], far)

    def hop_copy(p):
        return remote(("hop", p), t0.at[LX - p, halves[1], rows_z, :], relay.at[p], beside)

    def pass_copy(p):
        i, k = index.setdefault(("pass", p), len(index)), index[("far", p, 1)]
        return pltpu.make_async_remote_copy(
            src_ref=relay.at[p], dst_ref=t0.at[LX + 1 + p, halves[1], rows_z, :],
            send_sem=send_sem.at[i], recv_sem=recv_sem.at[k], device_id=diag, device_id_type=MESH)

    def near_copy(n):
        return remote(("near", n), t[n].at[1, pl.ds(1, LY), rows_z, :], t[n].at[0, pl.ds(1, LY), rows_z, :], near)

    def y_pair(name, n, ks):
        r = t[n]
        return [remote(name + ("lo",), r.at[ks, LY, rows_z, :], r.at[ks, 0, rows_z, :], yup),
                remote(name + ("hi",), r.at[ks, 1, rows_z, :], r.at[ks, LY + 1, rows_z, :], ydn)]

    def y_copies(n, j):
        return y_pair(("y", n, j), n, pl.ds(1 + CUTS[j], CUTS[j + 1] - CUTS[j]))

    def z_copies(n, j):
        ks = pl.ds(CUTS[j], CUTS[j + 1] - CUTS[j])
        return [remote(("z", n, j, "lo"), zsend.at[n, 0, ks], zrecv.at[n, 0, ks], zup),
                remote(("z", n, j, "hi"), zsend.at[n, 1, ks], zrecv.at[n, 1, ks], zdn)]

    def skew(p):
        return [(m, LX - 1 + p - m) for m in range(p + 1)]

    def skew_y(p):
        return [c for m, k in skew(p) for c in y_pair(("dy", p, m), m, k + 1)]

    def skew_z(p):
        ms = pl.ds(0, p + 1)
        return [remote(("dz", p, "lo"), dsend.at[p, 0, ms], drecv.at[p, 0, ms], zup),
                remote(("dz", p, "hi"), dsend.at[p, 1, ms], drecv.at[p, 1, ms], zdn)]

    def pot_copy(i):
        return remote(("pot", i), pot.at[plane(LX - 1 - i)], pot_halo.at[i], far)

    def ends(n, k):
        base = ((k + 1) * PY + 1) * PZ
        return flat[n][pl.ds(base + LZ - 1, LY, stride=PZ), :], flat[n][pl.ds(base, LY, stride=PZ), :]

    def set_ends(n, k, lo, hi):
        base = ((k + 1) * PY + 1) * PZ
        flat[n][pl.ds(base - 1, LY, stride=PZ), :] = lo
        flat[n][pl.ds(base + LZ, LY, stride=PZ), :] = hi

    def zpack(n, j):
        for k in range(CUTS[j], CUTS[j + 1]):
            zsend[n, 0, k], zsend[n, 1, k] = ends(n, k)

    def zunpack(n, j):
        for k in range(CUTS[j], CUTS[j + 1]):
            set_ends(n, k, zrecv[n, 0, k], zrecv[n, 1, k])

    def skew_pack(p):
        for m, k in skew(p):
            dsend[p, 0, m], dsend[p, 1, m] = ends(m, k)

    def skew_unpack(p):
        for m, k in skew(p):
            set_ends(m, k, drecv[p, 0, m], drecv[p, 1, m])

    def columns(n, k, ys, sums):
        cur, nxt = flat[n], flat[n + 1]
        for y in ys:
            base = pl.multiple_of(((k + 1) * PY + y + 1) * PZ, 8)
            c = cur[pl.ds(base, LZ), :]
            beside = cur[pl.ds(base - PY * PZ, LZ), :] + cur[pl.ds(base + PY * PZ, LZ), :]
            beside = beside + (cur[pl.ds(base - PZ, LZ), :] + cur[pl.ds(base + PZ, LZ), :])
            beside = beside + (cur[pl.ds(base - 1, LZ), :] + cur[pl.ds(base + 1, LZ), :])
            new = w[pl.ds(pl.multiple_of((k * LY + y) * LZ, 8), LZ), :] * c - (2.0 / 9.0) * beside
            if n == 0:
                new = 0.5 * new
            else:
                new = new - flat[n - 1][pl.ds(base, LZ), :]
            if n == ITERS - 1:
                nxt[pl.ds(pl.multiple_of((plane(k) * LY + y) * LZ, 8), LZ), :] = new
            else:
                nxt[pl.ds(base, LZ), :] = new
            if sums is not None:
                sums = (sums[0] + new * c, sums[1] + new * new, sums[2] + c * c if n == 0 else sums[2])
        return sums

    copies = []

    def send(cs):
        for c in cs:
            c.start()
            copies.append(c)

    def planes(n, lo, hi, ys, sums):
        return lax.fori_loop(lo, hi, lambda k, s: columns(n, k, ys, s), sums)

    def send_far(p):
        send([far_copy(p, 0)])
        direct = far_copy(p, 1)
        hop = hop_copy(p)

        @pl.when(edge)
        def _():
            hop.start()

        @pl.when(jnp.logical_not(edge))
        def _():
            direct.start()

    def forward(p):
        @pl.when(jnp.logical_not(edge))
        def _():
            hop_copy(p).wait_recv()
            pass_copy(p).start()

    def arrived(cs):
        for c in cs:
            c.wait_recv()

    send_far(0)
    for j in range(2):
        send(y_copies(0, j))
    send(skew_y(0) + [near_copy(0)])
    for j in range(2):
        zpack(0, j)
        send(z_copies(0, j))
    skew_pack(0)
    send(skew_z(0) + [pot_copy(i) for i in range(ITERS - 1)])

    pot_t = jnp.transpose(pot[...].reshape(LX * LY, LZ)) * (2.0 / 9.0)
    for x in range(LX):
        for y in range(LY):
            start = pl.multiple_of((plane(x) * LY + y) * LZ, 8)
            w[pl.ds(start, LZ), :] = jnp.broadcast_to(pot_t[:, x * LY + y:x * LY + y + 1], (LZ, R))
    forward(0)

    rows = [None] * 9
    outer, inner = (0, LY - 1), range(1, LY - 1)
    for n in range(ITERS):
        more = n < ITERS - 1
        zero = jnp.zeros((LZ, R), jnp.float32)
        sums = (zero, zero, zero)
        arrived(z_copies(n, 0) + [near_copy(n)] + y_copies(n, 0))
        zunpack(n, 0)
        sums = planes(n, CUTS[0], CUTS[1], outer, sums)
        if more:
            send(y_copies(n + 1, 0))
            send_far(n + 1)
        arrived(z_copies(n, 1) + y_copies(n, 1))
        zunpack(n, 1)
        sums = planes(n, CUTS[1], CUTS[2], outer, sums)
        if more:
            send(y_copies(n + 1, 1))
        sums = columns(n, 0, inner, sums)
        if more:
            send([near_copy(n + 1)])
        sums = planes(n, 1, CUTS[1], inner, sums)
        if more:
            zpack(n + 1, 0)
            send(z_copies(n + 1, 0))
        sums = planes(n, CUTS[1], CUTS[2], inner, sums)
        if more:
            zpack(n + 1, 1)
            send(z_copies(n + 1, 1))
        if n == 1:
            arrived([pot_copy(i) for i in range(ITERS - 1)])
            halo_t = jnp.transpose(pot_halo[...].reshape((ITERS - 1) * LY, LZ)) * (2.0 / 9.0)
            for i in range((ITERS - 1) * LY):
                start = (LX * LY + i) * LZ
                w[start:start + LZ, :] = jnp.broadcast_to(halo_t[:, i:i + 1], (LZ, R))
        arrived(skew_z(n) + skew_y(n))
        skew_unpack(n)
        if more:
            forward(n + 1)
        arrived([far_copy(n, 0), far_copy(n, 1)])
        for m, k in skew(n):
            if m < n:
                columns(m, k, range(LY), None)
            else:
                sums = columns(m, k, range(LY), sums)
        if more:
            send(skew_y(n + 1))
            skew_pack(n + 1)
            send(skew_z(n + 1))
        if n == 0:
            rows[0] = jnp.sum(sums[2], axis=0, keepdims=True)
        rows[2 * n + 1] = jnp.sum(sums[0], axis=0, keepdims=True)
        rows[2 * n + 2] = jnp.sum(sums[1], axis=0, keepdims=True)

    def gather(peers, buf, mine, ssem, rsem):
        outs = []
        for i, peer in enumerate(peers):
            c = pltpu.make_async_remote_copy(
                src_ref=part, dst_ref=buf.at[mine], send_sem=ssem.at[i], recv_sem=rsem.at[mine],
                device_id=peer, device_id_type=MESH)
            c.start()
            outs.append(c)
        return outs

    def arrive(slots, peers, buf, rsem, ssem):
        for slot, peer in zip(slots, peers):
            pltpu.make_async_remote_copy(
                src_ref=part, dst_ref=buf.at[slot], send_sem=ssem.at[0], recv_sem=rsem.at[slot],
                device_id=peer, device_id_type=MESH).wait_recv()

    part[...] = jnp.concatenate(rows, axis=0)
    bufa[mine_a] = part[...]
    outs = gather(peers_a, bufa, mine_a, asend, arecv)
    arrive([lax.rem(row_y + i // 4, 4) * 4 + lax.rem(gz + i % 4, 4) for i in range(1, 16)], peers_a, bufa, arecv, asend)
    for c in outs:
        c.wait_send()
    total = bufa[0]
    for i in range(1, 16):
        total = total + bufa[i]
    part[...] = total
    bufb[mine_b] = total
    outs = gather(peers_b, bufb, mine_b, bsend, brecv)
    arrive([lax.rem(row_z + i // 4, 4) * 4 + lax.rem(gx + i % 4, 4) for i in range(1, 16)], peers_b, bufb, brecv, bsend)
    for c in outs:
        c.wait_send()
    total = bufb[0]
    for i in range(1, 16):
        total = total + bufb[i]
    order = lax.broadcasted_iota(jnp.int32, (9, R), 0)
    base = jnp.where(order % 2 == 0, total[0:1, :], total[1:2, :])
    mom_ref[...] = jnp.where(order < 2, total, 2.0 * total - base) * (1.0 / SITES)
    for c in copies:
        c.wait_send()

    @pl.when(edge)
    def _():
        for p in range(ITERS):
            hop_copy(p).wait_send()

    @pl.when(jnp.logical_not(edge))
    def _():
        for p in range(ITERS):
            far_copy(p, 1).wait_send()
            pass_copy(p).wait_send()


def shards(random_vectors, potential):
    padded = pltpu.VMEM((PX, PY, PZ, R), jnp.float32)
    dma = pltpu.SemaphoreType.DMA
    return pl.pallas_call(
        kernel,
        out_shape=(jax.ShapeDtypeStruct((9, R), jnp.float32),
                   jax.ShapeDtypeStruct((LX, LY, LZ, R), jnp.float32)),
        in_specs=[pl.BlockSpec(memory_space=pltpu.MemorySpace.HBM)] * 2,
        out_specs=(pl.BlockSpec(memory_space=pltpu.VMEM), pl.BlockSpec(memory_space=pltpu.VMEM)),
        scratch_shapes=[padded] * 4 + [
            pltpu.VMEM(((LX + ITERS - 1) * LY * LZ, R), jnp.float32),
            pltpu.VMEM((LX, LY, LZ), jnp.float32),
            pltpu.VMEM((ITERS - 1, LY, LZ), jnp.float32),
            pltpu.VMEM((ITERS, 2, LX, LY, R), jnp.float32),
            pltpu.VMEM((ITERS, 2, LX, LY, R), jnp.float32),
            pltpu.VMEM((ITERS, 2, ITERS, LY, R), jnp.float32),
            pltpu.VMEM((ITERS, 2, ITERS, LY, R), jnp.float32),
            pltpu.VMEM((ITERS, LY // 2, LZ, R), jnp.float32),
            pltpu.VMEM((9, R), jnp.float32),
            pltpu.VMEM((16, 9, R), jnp.float32),
            pltpu.VMEM((16, 9, R), jnp.float32),
            dma((LX,)), dma, dma((COPIES,)), dma((COPIES,)),
            dma((16,)), dma((16,)), dma((16,)), dma((16,)),
        ],
        compiler_params=pltpu.CompilerParams(
            collective_id=0, has_side_effects=True, vmem_limit_bytes=LIMIT),
    )(pltpu.with_memory_space_constraint(random_vectors, pltpu.HBM), pltpu.with_memory_space_constraint(potential, pltpu.HBM))


def solution(mesh):
    placed = (P("gx", "gy", "gz", None), P("gx", "gy", "gz"))
    return jax.shard_map(
        shards, mesh=mesh, in_specs=placed, out_specs=(P(), P("gx", "gy", "gz", None)), check_vma=False)
```
